8 devices in a mesh: dp: 2 (over y, z), sp: 4 (over x, core).
Axes of the slice: x: 2, y: 2, z: 1, core: 2. Of those that a mesh axis runs over, the one named last changes fastest.
Arguments:
- x: bfloat16 [4096, 2048], P(('dp', 'sp')), parts along dimension 0
- gain: bfloat16 [2048], replicated
- wq: bfloat16 [2048, 2048], replicated
- wk: bfloat16 [2048, 2048], replicated
- wv: bfloat16 [2048, 2048], replicated
- wo: bfloat16 [2048, 2048], replicated
Outputs:
- output: bfloat16 [4096, 2048], P(('dp', 'sp')), parts along dimension 0
There are 2 independent parts. The reference program is written for one: setup_inputs(seed, part) draws one part's arguments, and reference() takes and returns one part's arrays. A program takes and returns all parts, laid end to end along the dimension named above; an argument that names none is the same for every part.
All inputs are finite; a program needn't handle non-finite values.
Results may differ from the reference program's by a relative error of at most 0.012.
Values are sent between devices in bfloat16 or wider.
A program may use at most 2 GiB of HBM per device.

```python
import jax
import jax.numpy as jnp
from jax import lax

ROWS = 2048
D = 2048
HEADS = 16
KV_HEADS = 16
HEAD = 128
THETA = 10000


def setup_inputs(seed: int = 0, part: int = 0) -> dict:
    kx, kn, kq, kk, kv, ko = jax.random.split(jax.random.key(seed), 6)

    def weights(key, rows, columns):
        return jax.random.normal(key, (rows, columns), jnp.float32) * rows**-0.5

    drawn = {
        "x": jax.random.normal(jax.random.fold_in(kx, part), (ROWS, D), jnp.float32),
        "gain": 1 + 0.1 * jax.random.normal(kn, (D,), jnp.float32),
        "wq": 2 * weights(kq, D, HEADS * HEAD),
        "wk": 2 * weights(kk, D, KV_HEADS * HEAD),
        "wv": 4 * weights(kv, D, KV_HEADS * HEAD),
        "wo": weights(ko, HEADS * HEAD, D),
    }
    return {k: v.astype(jnp.bfloat16) for k, v in drawn.items()}


def normed(x, gain):
    wide = x.astype(jnp.float32)
    scale = lax.rsqrt(jnp.mean(wide * wide, -1, keepdims=True) + 1e-6)
    return (wide * scale * gain.astype(jnp.float32)).astype(jnp.bfloat16)


def turned(t, place, theta):
    half = t.shape[-1] // 2
    angle = place.astype(jnp.float32)[:, None] * theta ** (-jnp.arange(half, dtype=jnp.float32) / half)
    cos, sin = jnp.cos(angle)[:, None], jnp.sin(angle)[:, None]
    a, b = t[..., :half].astype(jnp.float32), t[..., half:].astype(jnp.float32)
    return jnp.concatenate([a * cos - b * sin, b * cos + a * sin], -1).astype(jnp.bfloat16)


def matmul(a, w):
    return jnp.dot(a, w, preferred_element_type=jnp.float32).astype(jnp.bfloat16)


def einsum(form, a, b):
    return jnp.einsum(form, a.astype(jnp.float32), b.astype(jnp.float32))


def attention(q, k, v):
    scores = einsum("tgsd,ugd->gstu", q, k) * q.shape[-1] ** -0.5
    token = jnp.arange(q.shape[0])
    scores = jnp.where(token[:, None] >= token, scores, -jnp.inf)
    weights = jax.nn.softmax(scores, -1).astype(jnp.bfloat16)
    return einsum("gstu,ugd->tgsd", weights, v).astype(jnp.bfloat16)


def reference(x, gain, wq, wk, wv, wo):
    a, place = normed(x, gain), jnp.arange(ROWS)
    q = turned(matmul(a, wq).reshape(ROWS, HEADS, HEAD), place, THETA).reshape(ROWS, KV_HEADS, -1, HEAD)
    k = turned(matmul(a, wk).reshape(ROWS, KV_HEADS, HEAD), place, THETA)
    v = matmul(a, wv).reshape(ROWS, KV_HEADS, HEAD)
    seen = attention(q, k, v).reshape(ROWS, HEADS * HEAD)
    return (x.astype(jnp.float32) + jnp.dot(seen, wo, preferred_element_type=jnp.float32)).astype(jnp.bfloat16)
```

```python
import functools

import jax
import jax.numpy as jnp
import numpy as np
from jax import lax
from jax.experimental import pallas as pl
from jax.experimental.pallas import tpu as pltpu
from jax.sharding import PartitionSpec as P

HEAD = 128
THETA = 10000
PAIR = 2 * HEAD
LOG2E = 1.4426950408889634
E = HEAD**-0.5 * LOG2E
HIDDEN = -1e30
F32, BF16 = jnp.float32, jnp.bfloat16
MESH = pl.DeviceIdType.MESH


def dot(a, b):
    return jnp.dot(a, b, preferred_element_type=F32)


def attend(q, parts):
    scores = []
    for k, _, causal in parts:
        s = dot(k, q)
        if causal:
            s = jnp.where(lax.broadcasted_iota(jnp.int32, s.shape, 0) <= lax.broadcasted_iota(jnp.int32, s.shape, 1), s, HIDDEN)
        scores.append(s)
    top = functools.reduce(jnp.maximum, [s.max(axis=0, keepdims=True) for s in scores])
    total, out = 0, 0
    for s, (_, v, _) in zip(scores, parts):
        p = jnp.exp2((s - top) * E)
        total = total + p.sum(axis=0, keepdims=True)
        out = out + dot(v, p.astype(BF16))
    return out, top * E, total


def kernel(x_hbm, gain_ref, turn_hbm, wq_hbm, wk_hbm, wv_hbm, wo_hbm, y_hbm, xv, av, wq, wk, wv, wo, ks, vs, qs, inbox, outbox, lin, lout, acc, turn, part,
           tops, sums, seen, w_sem, m_sem, xs, xr, ls, lr, kss, ksr, vss, vsr):
    own, pairs = xv.shape[0], wq.shape[0]
    me = lax.axis_index("sp")
    chip, core = lax.div(me, 2), lax.rem(me, 2)
    sibling = 2 * chip + 1 - core
    first, second = chip == 0, chip == 1
    half = own // 2

    barrier = pltpu.get_barrier_semaphore()
    others = [lax.rem(me + n, 4) for n in (1, 2, 3)]
    for other in others:
        pl.semaphore_signal(barrier, inc=1, device_id={"sp": other}, device_id_type=MESH)

    def columns(w_hbm, w, i, hp):
        return pltpu.make_async_copy(w_hbm.at[:, pl.ds(pl.multiple_of(hp * PAIR, PAIR), PAIR)], w.at[hp], w_sem.at[i, hp])

    def rows(hp):
        return pltpu.make_async_copy(wo_hbm.at[pl.ds(pl.multiple_of(hp * PAIR, PAIR), PAIR), :], wo.at[hp], w_sem.at[3, hp])

    get_q, get_k, get_v = (functools.partial(columns, *t) for t in ((wq_hbm, wq, 0), (wk_hbm, wk, 1), (wv_hbm, wv, 2)))
    get_x = pltpu.make_async_copy(x_hbm, xv, m_sem.at[0])
    get_turn = pltpu.make_async_copy(turn_hbm.at[pl.ds(pl.multiple_of(me * own, own), own), :], turn.at[0], m_sem.at[1])
    get_x.start()
    get_turn.start()

    def start_all(*gets):
        def body(hp, _):
            for get in gets:
                get(hp).start()
        lax.fori_loop(0, pairs, body, None)

    @pl.when(first)
    def _():
        start_all(get_k, get_v)
        start_all(get_q)

    @pl.when(second)
    def _():
        start_all(get_q)
        start_all(get_k, get_v)

    start_all(rows)

    get_x.wait()

    def norm(i, _):
        at = pl.ds(pl.multiple_of(i * 64, 64), 64)
        wide = xv[at, :].astype(F32)
        scale = lax.rsqrt(jnp.mean(wide * wide, -1, keepdims=True) + 1e-6)
        av[at, :] = (wide * scale * gain_ref[...].astype(F32)).astype(BF16)
        acc[at, :] = wide

    lax.fori_loop(0, own // 64, norm, None)

    get_turn.wait()
    table = turn[0]
    swapped = pltpu.roll(table, HEAD // 2, 1)
    low = lax.broadcasted_iota(jnp.int32, table.shape, 1) < HEAD // 2
    turn[0] = jnp.where(low, table, swapped)
    turn[1] = jnp.where(low, -swapped, table)

    pl.semaphore_wait(barrier, 3)

    def turned(t):
        wide = t.astype(F32)
        return (wide * turn[0] + pltpu.roll(wide, HEAD // 2, 1) * turn[1]).astype(BF16)

    def remote(src, dst, send, recv, device):
        return pltpu.make_async_remote_copy(src_ref=src, dst_ref=dst, send_sem=send, recv_sem=recv, device_id={"sp": device}, device_id_type=MESH)

    def send_query(hp, j):
        return remote(qs.at[hp, j], inbox.at[hp, core], xs.at[hp, j], xr.at[hp, core], j)

    def send_part(hp, j):
        return remote(outbox.at[hp, j], inbox.at[hp, core], xs.at[hp, j], xr.at[hp, core], 2 + j)

    def send_sum(hp, j):
        return remote(lout.at[hp, j], lin.at[hp, core], ls.at[hp, j], lr.at[hp, core], 2 + j)

    def got(hp, j):
        return remote(inbox.at[hp, j], inbox.at[hp, j], xs.at[hp, j], xr.at[hp, j], 2 * (1 - chip) + j)

    def got_sum(hp, j):
        return remote(lin.at[hp, j], lin.at[hp, j], ls.at[hp, j], lr.at[hp, j], 2 * (1 - chip) + j)

    def send_keys(hp):
        return remote(ks.at[hp, core], ks.at[hp, core], kss.at[hp], ksr.at[hp], sibling)

    def send_values(hp):
        return remote(vs.at[hp, core], vs.at[hp, core], vss.at[hp], vsr.at[hp], sibling)

    sends_keys, gets_keys = first | (core == 0), first | (core == 1)

    def query(hp):
        get_q(hp).wait()
        t = dot(av[...], wq[hp]).astype(BF16)
        for h in range(2):
            qs[hp, h] = turned(t[:, h * HEAD : (h + 1) * HEAD]).T

    def key_value(hp, _):
        get_k(hp).wait()
        get_v(hp).wait()
        t = dot(av[...], wk[hp]).astype(BF16)
        for h in range(2):
            ks[hp, core, h] = turned(t[:, h * HEAD : (h + 1) * HEAD])
        t = dot(av[...], wv[hp]).astype(BF16)
        for h in range(2):
            vs[hp, core, h] = t[:, h * HEAD : (h + 1) * HEAD].T

        @pl.when(sends_keys)
        def _():
            send_keys(hp).start()
            send_values(hp).start()

    @pl.when(second)
    def _():
        def body(hp, _):
            query(hp)
            for j in range(2):
                send_query(hp, j).start()
        lax.fori_loop(0, pairs, body, None)

    lax.fori_loop(0, pairs, key_value, None)

    def own_part(hp, before):
        for h in range(2):
            for n in range(2):
                at = slice(n * half, (n + 1) * half)
                parts = [(ks[hp, 0, h], vs[hp, 0, h], False)] if before else []
                mine = int(before)
                if n:
                    parts.append((ks[hp, mine, h, :half], vs[hp, mine, h, :, :half], False))
                parts.append((ks[hp, mine, h, at], vs[hp, mine, h, :, at], True))
                part[h, :, at], tops[h, :, at], sums[h, :, at] = attend(qs[hp, h, :, at], parts)

    def pair(hp, _):
        @pl.when(gets_keys)
        def _():
            send_keys(hp).wait_recv()
            send_values(hp).wait_recv()

        @pl.when(first)
        def _():
            for j in range(2):
                got(hp, j).wait_recv()
                out, top, total = attend(inbox[hp, j], [(ks[hp, n, core], vs[hp, n, core], False) for n in range(2)])
                outbox[hp, j] = (out * (1 / total)).astype(BF16)
                lout[hp, j] = top + jnp.log2(total)
                send_part(hp, j).start()
                send_sum(hp, j).start()
            query(hp)

        @pl.when(core == 0)
        def _():
            own_part(hp, False)

        @pl.when(core == 1)
        def _():
            own_part(hp, True)

        @pl.when(first)
        def _():
            for h in range(2):
                seen[:, h * HEAD : (h + 1) * HEAD] = (part[h] * (1 / sums[h])).T.astype(BF16)

        @pl.when(second)
        def _():
            for h in range(2):
                got(hp, h).wait_recv()
                got_sum(hp, h).wait_recv()
                here, there = tops[h] + jnp.log2(sums[h]), lin[hp, h]
                top = jnp.maximum(here, there)
                a, b = jnp.exp2(here - top), jnp.exp2(there - top)
                both = part[h] * (a / (sums[h] * (a + b))) + inbox[hp, h].astype(F32) * (b / (a + b))
                seen[:, h * HEAD : (h + 1) * HEAD] = both.T.astype(BF16)

        rows(hp).wait()
        for n in range(0, acc.shape[1], 512):
            acc[:, n : n + 512] += dot(seen[...], wo[hp, :, n : n + 512])

    lax.fori_loop(0, pairs, pair, None)

    xv[...] = acc[...].astype(BF16)
    put = pltpu.make_async_copy(xv, y_hbm, m_sem.at[0])
    put.start()

    def finish(hp, _):
        @pl.when(sends_keys)
        def _():
            send_keys(hp).wait_send()
            send_values(hp).wait_send()

        for j in range(2):
            @pl.when(first)
            def _():
                send_part(hp, j).wait_send()
                send_sum(hp, j).wait_send()

            @pl.when(second)
            def _():
                send_query(hp, j).wait_send()

    lax.fori_loop(0, pairs, finish, None)
    put.wait()


def turning(tokens):
    half = HEAD // 2
    angle = np.arange(tokens)[:, None] * float(THETA) ** (-np.arange(half) / half)
    return np.concatenate([np.cos(angle), np.sin(angle)], -1).astype(np.float32)


def solution(mesh):
    devices = mesh.shape["sp"]

    def step(x, gain, wq, wk, wv, wo):
        own, width = x.shape
        pairs = wq.shape[1] // PAIR
        anywhere, vmem = pl.BlockSpec(memory_space=pl.ANY), pl.BlockSpec(memory_space=pltpu.VMEM)
        dma = lambda *shape: pltpu.SemaphoreType.DMA(shape)
        flops = 2 * own * width * 4 * width + 4 * own * own * devices * width
        return pl.pallas_call(
            kernel,
            out_shape=jax.ShapeDtypeStruct((own, width), BF16),
            in_specs=[anywhere, vmem] + [anywhere] * 5,
            out_specs=anywhere,
            scratch_shapes=[
                pltpu.VMEM((own, width), BF16),
                pltpu.VMEM((own, width), BF16),
                pltpu.VMEM((pairs, width, PAIR), BF16),
                pltpu.VMEM((pairs, width, PAIR), BF16),
                pltpu.VMEM((pairs, width, PAIR), BF16),
                pltpu.VMEM((pairs, PAIR, width), BF16),
                pltpu.VMEM((pairs, 2, 2, own, HEAD), BF16),
                pltpu.VMEM((pairs, 2, 2, HEAD, own), BF16),
                pltpu.VMEM((pairs, 2, HEAD, own), BF16),
                pltpu.VMEM((pairs, 2, HEAD, own), BF16),
                pltpu.VMEM((pairs, 2, HEAD, own), BF16),
                pltpu.VMEM((pairs, 2, 1, own), F32),
                pltpu.VMEM((pairs, 2, 1, own), F32),
                pltpu.VMEM((own, width), F32),
                pltpu.VMEM((2, own, HEAD), F32),
                pltpu.VMEM((2, HEAD, own), F32),
                pltpu.VMEM((2, 1, own), F32),
                pltpu.VMEM((2, 1, own), F32),
                pltpu.VMEM((own, PAIR), BF16),
                dma(4, pairs), dma(2), dma(pairs, 2), dma(pairs, 2), dma(pairs, 2), dma(pairs, 2), dma(pairs), dma(pairs), dma(pairs), dma(pairs),
            ],
            compiler_params=pltpu.CompilerParams(collective_id=0, has_side_effects=True, vmem_limit_bytes=67043328),
            cost_estimate=pl.CostEstimate(flops=flops, transcendentals=own * own * 2 * pairs * 2, bytes_accessed=4 * width * width * 2),
        )(x, gain.reshape(1, -1), jnp.asarray(turning(devices * own)), wq, wk, wv, wo)

    tokens, whole = P(("dp", "sp"), None), P(None, None)
    return jax.shard_map(
        step,
        mesh=mesh,
        in_specs=(tokens, P(None), whole, whole, whole, whole),
        out_specs=tokens,
        check_vma=False,
    )
```

```python
import functools

import jax
import jax.numpy as jnp
import numpy as np
from jax import lax
from jax.experimental import pallas as pl
from jax.experimental.pallas import tpu as pltpu
from jax.sharding import PartitionSpec as P

HEAD = 128
THETA = 10000
PAIR = 2 * HEAD
LOG2E = 1.4426950408889634
E = HEAD**-0.5 * LOG2E
HIDDEN = -1e30
CHUNK = 64
F32, BF16 = jnp.float32, jnp.bfloat16
MESH = pl.DeviceIdType.MESH


def dot(a, b):
    return jnp.dot(a, b, preferred_element_type=F32)


def scores(q, parts):
    found = []
    for k, _, causal in parts:
        s = dot(k, q)
        if causal:
            s = jnp.where(lax.broadcasted_iota(jnp.int32, s.shape, 0) <= lax.broadcasted_iota(jnp.int32, s.shape, 1), s, HIDDEN)
        found.append(s)
    return found


def attend(strips):
    found = [scores(q, parts) for q, parts, _ in strips]
    tops = [functools.reduce(jnp.maximum, [s.max(axis=0, keepdims=True) for s in mine]) for mine in found]
    weights = [[jnp.exp2((s - top) * E).astype(BF16) for s in mine] for mine, top in zip(found, tops)]
    for (_, parts, put), top, mine in zip(strips, tops, weights):
        out = sum(dot(jnp.concatenate([v, jnp.ones((8, v.shape[1]), BF16)], axis=0), p) for (_, v, _), p in zip(parts, mine))
        put(out[:HEAD], top * E, out[HEAD : HEAD + 1])


def kernel(x_hbm, gain_ref, turn_hbm, wq_hbm, wk_hbm, wv_hbm, wo_hbm, y_hbm, xv, av, wq, wk, wv, wo, ks, vs, qs, inbox, outbox, lin, lout, acc, turn, part,
           tops, sums, seen, w_sem, x_sem, m_sem, xs, xr, ls, lr, kss, ksr, vss, vsr):
    own, pairs = xv.shape[0], wq.shape[0]
    me = lax.axis_index("sp")
    chip, core = lax.div(me, 2), lax.rem(me, 2)
    sibling = 2 * chip + 1 - core
    first, second = chip == 0, chip == 1
    half = own // 2

    barrier = pltpu.get_barrier_semaphore()
    others = [lax.rem(me + n, 4) for n in (1, 2, 3)]
    for other in others:
        pl.semaphore_signal(barrier, inc=1, device_id={"sp": other}, device_id_type=MESH)

    def columns(w_hbm, w, i, hp):
        return pltpu.make_async_copy(w_hbm.at[:, pl.ds(pl.multiple_of(hp * PAIR, PAIR), PAIR)], w.at[hp], w_sem.at[i, hp])

    def rows(hp):
        return pltpu.make_async_copy(wo_hbm.at[pl.ds(pl.multiple_of(hp * PAIR, PAIR), PAIR), :], wo.at[hp], w_sem.at[3, hp])

    get_q, get_k, get_v = (functools.partial(columns, *t) for t in ((wq_hbm, wq, 0), (wk_hbm, wk, 1), (wv_hbm, wv, 2)))
    def get_x(i):
        at = pl.ds(pl.multiple_of(i * CHUNK, CHUNK), CHUNK)
        return pltpu.make_async_copy(x_hbm.at[at, :], xv.at[at, :], x_sem.at[i])

    get_turn = pltpu.make_async_copy(turn_hbm.at[pl.ds(pl.multiple_of(me * own, own), own), :], turn.at[0], m_sem.at[1])
    for i in range(own // CHUNK):
        get_x(i).start()
    get_turn.start()

    def start_all(*gets):
        def body(hp, _):
            for get in gets:
                get(hp).start()
        lax.fori_loop(0, pairs, body, None)

    @pl.when(first)
    def _():
        start_all(get_k, get_v)
        start_all(get_q)

    @pl.when(second)
    def _():
        start_all(get_q)
        start_all(get_k, get_v)

    start_all(rows)

    def norm(i, _):
        get_x(i).wait()
        at = pl.ds(pl.multiple_of(i * CHUNK, CHUNK), CHUNK)
        wide = xv[at, :].astype(F32)
        scale = lax.rsqrt(jnp.mean(wide * wide, -1, keepdims=True) + 1e-6)
        av[at, :] = (wide * scale * gain_ref[...].astype(F32).reshape(1, -1)).astype(BF16)
        acc[at, :] = wide

    lax.fori_loop(0, own // CHUNK, norm, None)

    get_turn.wait()
    table = turn[0]
    swapped = pltpu.roll(table, HEAD // 2, 1)
    low = lax.broadcasted_iota(jnp.int32, table.shape, 1) < HEAD // 2
    turn[0] = jnp.where(low, table, swapped)
    turn[1] = jnp.where(low, -swapped, table)

    pl.semaphore_wait(barrier, 3)

    def turned(t):
        wide = t.astype(F32)
        return (wide * turn[0] + pltpu.roll(wide, HEAD // 2, 1) * turn[1]).astype(BF16)

    def remote(src, dst, send, recv, device):
        return pltpu.make_async_remote_copy(src_ref=src, dst_ref=dst, send_sem=send, recv_sem=recv, device_id={"sp": device}, device_id_type=MESH)

    def send_query(hp, j):
        return remote(qs.at[hp, j], inbox.at[hp, core], xs.at[hp, j], xr.at[hp, core], j)

    def send_part(hp, j):
        return remote(outbox.at[hp, j], inbox.at[hp, core], xs.at[hp, j], xr.at[hp, core], 2 + j)

    def send_sum(hp, j):
        return remote(lout.at[hp, j], lin.at[hp, core], ls.at[hp, j], lr.at[hp, core], 2 + j)

    def got(hp, j):
        return remote(inbox.at[hp, j], inbox.at[hp, j], xs.at[hp, j], xr.at[hp, j], 2 * (1 - chip) + j)

    def got_sum(hp, j):
        return remote(lin.at[hp, j], lin.at[hp, j], ls.at[hp, j], lr.at[hp, j], 2 * (1 - chip) + j)

    def send_keys(hp):
        return remote(ks.at[hp, core], ks.at[hp, core], kss.at[hp], ksr.at[hp], sibling)

    def send_values(hp):
        return remote(vs.at[hp, core], vs.at[hp, core], vss.at[hp], vsr.at[hp], sibling)

    sends_keys = first | (core == 0)

    def query(hp):
        get_q(hp).wait()
        t = dot(av[...], wq[hp]).astype(BF16)
        for h in range(2):
            qs[hp, h] = turned(t[:, h * HEAD : (h + 1) * HEAD]).T

    def key_value(hp, _):
        get_k(hp).wait()
        get_v(hp).wait()
        t = dot(av[...], wk[hp]).astype(BF16)
        for h in range(2):
            ks[hp, core, h] = turned(t[:, h * HEAD : (h + 1) * HEAD])
        t = dot(av[...], wv[hp]).astype(BF16)
        for h in range(2):
            vs[hp, core, h] = t[:, h * HEAD : (h + 1) * HEAD].T

        @pl.when(sends_keys)
        def _():
            send_keys(hp).start()
            send_values(hp).start()

    def own_part(hp, before):
        strips = []
        for h in range(2):
            for n in range(2):
                at = slice(n * half, (n + 1) * half)
                parts = [(ks[hp, 0, h], vs[hp, 0, h], False)] if before else []
                mine = int(before)
                if n:
                    parts.append((ks[hp, mine, h, :half], vs[hp, mine, h, :, :half], False))
                parts.append((ks[hp, mine, h, at], vs[hp, mine, h, :, at], True))

                def put(out, top, total, h=h, at=at):
                    part[h, :, at], tops[h, :, at], sums[h, :, at] = out, top, total

                strips.append((qs[hp, h, :, at], parts, put))
        attend(strips)

    def other_part(hp):
        strips = []
        for j in range(2):
            for n in range(2):
                at = slice(n * half, (n + 1) * half)

                def put(out, top, total, j=j, at=at):
                    outbox[hp, j, :, at] = (out * (1 / total)).astype(BF16)
                    lout[hp, j, :, at] = top + jnp.log2(total)

                strips.append((inbox[hp, j, :, at], [(ks[hp, n, core], vs[hp, n, core], False) for n in range(2)], put))
        attend(strips)

    def own_parts(hp):
        @pl.when(core == 0)
        def _():
            own_part(hp, False)

        @pl.when(core == 1)
        def _():
            own_part(hp, True)

    def project(hp):
        rows(hp).wait()
        for n in range(0, acc.shape[1], 512):
            acc[:, n : n + 512] += dot(seen[...], wo[hp, :, n : n + 512])

    @pl.when(first)
    def _():
        ahead = pairs - 2
        late = 1
        lax.fori_loop(0, ahead, key_value, None)

        def body(t, _):
            @pl.when(t < pairs)
            def _():
                send_keys(t).wait_recv()
                send_values(t).wait_recv()
                for j in range(2):
                    got(t, j).wait_recv()
                other_part(t)
                for j in range(2):
                    send_part(t, j).start()
                    send_sum(t, j).start()

            @pl.when(t < late)
            def _():
                each = (pairs - ahead) // late
                lax.fori_loop(0, each, lambda i, _: key_value(ahead + t * each + i, _), None)

            @pl.when(t >= late)
            def _():
                hp = t - late
                query(hp)
                own_parts(hp)
                for h in range(2):
                    seen[:, h * HEAD : (h + 1) * HEAD] = (part[h] * (1 / sums[h])).T.astype(BF16)
                project(hp)

        lax.fori_loop(0, pairs + late, body, None)

    @pl.when(second)
    def _():
        def ask(hp, _):
            query(hp)
            for j in range(2):
                send_query(hp, j).start()

        lax.fori_loop(0, pairs, ask, None)
        lax.fori_loop(0, pairs, key_value, None)

        def body(hp, _):
            @pl.when(core == 1)
            def _():
                send_keys(hp).wait_recv()
                send_values(hp).wait_recv()

            own_parts(hp)
            for h in range(2):
                got(hp, h).wait_recv()
                got_sum(hp, h).wait_recv()
                here, there = tops[h] + jnp.log2(sums[h]), lin[hp, h]
                top = jnp.maximum(here, there)
                a, b = jnp.exp2(here - top), jnp.exp2(there - top)
                both = part[h] * (a / (sums[h] * (a + b))) + inbox[hp, h].astype(F32) * (b / (a + b))
                seen[:, h * HEAD : (h + 1) * HEAD] = both.T.astype(BF16)
            project(hp)

        lax.fori_loop(0, pairs, body, None)

    xv[...] = acc[...].astype(BF16)
    put = pltpu.make_async_copy(xv, y_hbm, m_sem.at[0])
    put.start()

    def finish(hp, _):
        @pl.when(sends_keys)
        def _():
            send_keys(hp).wait_send()
            send_values(hp).wait_send()

        for j in range(2):
            @pl.when(first)
            def _():
                send_part(hp, j).wait_send()
                send_sum(hp, j).wait_send()

            @pl.when(second)
            def _():
                send_query(hp, j).wait_send()

    lax.fori_loop(0, pairs, finish, None)
    put.wait()


def turning(tokens):
    half = HEAD // 2
    angle = np.arange(tokens)[:, None] * float(THETA) ** (-np.arange(half) / half)
    return np.concatenate([np.cos(angle), np.sin(angle)], -1).astype(np.float32)


def solution(mesh):
    devices = mesh.shape["sp"]

    def step(x, gain, wq, wk, wv, wo):
        own, width = x.shape
        pairs = wq.shape[1] // PAIR
        anywhere, vmem = pl.BlockSpec(memory_space=pl.ANY), pl.BlockSpec(memory_space=pltpu.VMEM)
        dma = lambda *shape: pltpu.SemaphoreType.DMA(shape)
        flops = 2 * own * width * 4 * width + 4 * own * own * devices * width
        return pl.pallas_call(
            kernel,
            out_shape=jax.ShapeDtypeStruct((own, width), BF16),
            in_specs=[anywhere, vmem] + [anywhere] * 5,
            out_specs=anywhere,
            scratch_shapes=[
                pltpu.VMEM((own, width), BF16),
                pltpu.VMEM((own, width), BF16),
                pltpu.VMEM((pairs, width, PAIR), BF16),
                pltpu.VMEM((pairs, width, PAIR), BF16),
                pltpu.VMEM((pairs, width, PAIR), BF16),
                pltpu.VMEM((pairs, PAIR, width), BF16),
                pltpu.VMEM((pairs, 2, 2, own, HEAD), BF16),
                pltpu.VMEM((pairs, 2, 2, HEAD, own), BF16),
                pltpu.VMEM((pairs, 2, HEAD, own), BF16),
                pltpu.VMEM((pairs, 2, HEAD, own), BF16),
                pltpu.VMEM((pairs, 2, HEAD, own), BF16),
                pltpu.VMEM((pairs, 2, 1, own), F32),
                pltpu.VMEM((pairs, 2, 1, own), F32),
                pltpu.VMEM((own, width), F32),
                pltpu.VMEM((2, own, HEAD), F32),
                pltpu.VMEM((2, HEAD, own), F32),
                pltpu.VMEM((2, 1, own), F32),
                pltpu.VMEM((2, 1, own), F32),
                pltpu.VMEM((own, PAIR), BF16),
                dma(4, pairs), dma(own // CHUNK), dma(2), dma(pairs, 2), dma(pairs, 2), dma(pairs, 2), dma(pairs, 2), dma(pairs), dma(pairs), dma(pairs), dma(pairs),
            ],
            compiler_params=pltpu.CompilerParams(collective_id=0, has_side_effects=True, vmem_limit_bytes=67043328),
            cost_estimate=pl.CostEstimate(flops=flops, transcendentals=own * own * 2 * pairs * 2, bytes_accessed=4 * width * width * 2),
        )(x, gain, jnp.asarray(turning(devices * own)), wq, wk, wv, wo)

    tokens, whole = P(("dp", "sp"), None), P(None, None)
    return jax.shard_map(
        step,
        mesh=mesh,
        in_specs=(tokens, P(None), whole, whole, whole, whole),
        out_specs=tokens,
        check_vma=False,
    )
```

```python
import functools

import jax
import jax.numpy as jnp
import numpy as np
from jax import lax
from jax.experimental import pallas as pl
from jax.experimental.pallas import tpu as pltpu
from jax.sharding import PartitionSpec as P

HEAD = 128
THETA = 10000
PAIR = 2 * HEAD
LOG2E = 1.4426950408889634
E = HEAD**-0.5 * LOG2E
HIDDEN = -1e30
CHUNK = 64
F32, BF16 = jnp.float32, jnp.bfloat16
MESH = pl.DeviceIdType.MESH


def dot(a, b):
    return jnp.dot(a, b, preferred_element_type=F32)


def scores(q, parts):
    found = []
    for k, _, causal in parts:
        s = dot(k, q)
        if causal:
            s = jnp.where(lax.broadcasted_iota(jnp.int32, s.shape, 0) <= lax.broadcasted_iota(jnp.int32, s.shape, 1), s, HIDDEN)
        found.append(s)
    return found


def attend(strips):
    found = [scores(q, parts) for q, parts, _ in strips]
    tops = [functools.reduce(jnp.maximum, [s.max(axis=0, keepdims=True) for s in mine]) for mine in found]
    weights = [[jnp.exp2((s - top) * E).astype(BF16) for s in mine] for mine, top in zip(found, tops)]
    for (_, parts, put), top, mine in zip(strips, tops, weights):
        out = sum(dot(jnp.concatenate([v, jnp.ones((8, v.shape[1]), BF16)], axis=0), p) for (_, v, _), p in zip(parts, mine))
        put(out[:HEAD], top * E, out[HEAD : HEAD + 1])


def kernel(x_hbm, gain_hbm, turn_hbm, wq_hbm, wk_hbm, wv_hbm, wo_hbm, y_ref, xv, av, gv, wq, wk, wv, wo, ks, vs, qs, inbox, outbox, lin, lout, acc, turn, part,
           tops, sums, seen, w_sem, x_sem, m_sem, xs, xr, ls, lr, kss, ksr, vss, vsr, kx, vx, cs, cr, fs, fr):
    own, pairs = xv.shape[0], wq.shape[0]
    me = lax.axis_index("sp")
    chip, core = lax.div(me, 2), lax.rem(me, 2)
    sibling = 2 * chip + 1 - core
    first, second = chip == 0, chip == 1
    half = own // 2

    barrier = pltpu.get_barrier_semaphore()
    others = [lax.rem(me + n, 4) for n in (1, 2, 3)]
    for other in others:
        pl.semaphore_signal(barrier, inc=1, device_id={"sp": other}, device_id_type=MESH)

    def columns(w_hbm, w, i, hp):
        return pltpu.make_async_copy(w_hbm.at[:, pl.ds(pl.multiple_of(hp * PAIR, PAIR), PAIR)], w.at[hp], w_sem.at[i, hp])

    def rows(hp):
        return pltpu.make_async_copy(wo_hbm.at[pl.ds(pl.multiple_of(hp * PAIR, PAIR), PAIR), :], wo.at[hp], w_sem.at[3, hp])

    get_q, get_k, get_v = (functools.partial(columns, *t) for t in ((wq_hbm, wq, 0), (wk_hbm, wk, 1), (wv_hbm, wv, 2)))
    def get_x(i):
        at = pl.ds(pl.multiple_of(i * CHUNK, CHUNK), CHUNK)
        return pltpu.make_async_copy(x_hbm.at[at, :], xv.at[at, :], x_sem.at[i])

    get_turn = pltpu.make_async_copy(turn_hbm.at[pl.ds(pl.multiple_of(me * own, own), own), :], turn.at[0], m_sem.at[1])
    for i in range(own // CHUNK):
        get_x(i).start()
    get_gain = pltpu.make_async_copy(gain_hbm, gv, m_sem.at[0])
    get_gain.start()
    get_turn.start()

    def start_all(count, *gets):
        def body(hp, _):
            for get in gets:
                get(hp).start()
        lax.fori_loop(0, count, body, None)

    @pl.when(first)
    def _():
        for get in (get_k, get_v):
            get(pairs - 1).start()
        start_all(pairs - 1, get_k, get_v)
        start_all(pairs, get_q)

    @pl.when(second)
    def _():
        start_all(pairs, get_q)
        start_all(pairs, get_k, get_v)

    start_all(pairs, rows)

    get_gain.wait()

    def norm(i, _):
        get_x(i).wait()
        at = pl.ds(pl.multiple_of(i * CHUNK, CHUNK), CHUNK)
        wide = xv[at, :].astype(F32)
        scale = lax.rsqrt(jnp.mean(wide * wide, -1, keepdims=True) + 1e-6)
        av[at, :] = (wide * scale * gv[...].astype(F32).reshape(1, -1)).astype(BF16)
        acc[at, :] = wide

    lax.fori_loop(0, own // CHUNK, norm, None)

    get_turn.wait()
    table = turn[0]
    swapped = pltpu.roll(table, HEAD // 2, 1)
    low = lax.broadcasted_iota(jnp.int32, table.shape, 1) < HEAD // 2
    turn[0] = jnp.where(low, table, swapped)
    turn[1] = jnp.where(low, -swapped, table)

    pl.semaphore_wait(barrier, 3)

    def turned(t):
        wide = t.astype(F32)
        return (wide * turn[0] + pltpu.roll(wide, HEAD // 2, 1) * turn[1]).astype(BF16)

    def remote(src, dst, send, recv, device):
        return pltpu.make_async_remote_copy(src_ref=src, dst_ref=dst, send_sem=send, recv_sem=recv, device_id={"sp": device}, device_id_type=MESH)

    def send_query(hp, j):
        return remote(qs.at[hp, j], inbox.at[hp, core], xs.at[hp, j], xr.at[hp, core], j)

    def send_part(hp, j):
        return remote(outbox.at[hp, j], inbox.at[hp, core], xs.at[hp, j], xr.at[hp, core], 2 + j)

    def send_sum(hp, j):
        return remote(lout.at[hp, j], lin.at[hp, core], ls.at[hp, j], lr.at[hp, core], 2 + j)

    def got(hp, j):
        return remote(inbox.at[hp, j], inbox.at[hp, j], xs.at[hp, j], xr.at[hp, j], 2 * (1 - chip) + j)

    def got_sum(hp, j):
        return remote(lin.at[hp, j], lin.at[hp, j], ls.at[hp, j], lr.at[hp, j], 2 * (1 - chip) + j)

    def send_keys(hp):
        return remote(ks.at[hp, core], ks.at[hp, core], kss.at[hp], ksr.at[hp], sibling)

    def send_values(hp):
        return remote(vs.at[hp, core], vs.at[hp, core], vss.at[hp], vsr.at[hp], sibling)

    sends_keys = first | (core == 0)

    def query(hp):
        get_q(hp).wait()
        t = dot(av[...], wq[hp]).astype(BF16)
        for h in range(2):
            qs[hp, h] = turned(t[:, h * HEAD : (h + 1) * HEAD]).T

    def key_value(hp, _):
        get_k(hp).wait()
        get_v(hp).wait()
        t = dot(av[...], wk[hp]).astype(BF16)
        for h in range(2):
            ks[hp, core, h] = turned(t[:, h * HEAD : (h + 1) * HEAD])
        t = dot(av[...], wv[hp]).astype(BF16)
        for h in range(2):
            vs[hp, core, h] = t[:, h * HEAD : (h + 1) * HEAD].T

        @pl.when(sends_keys)
        def _():
            send_keys(hp).start()
            send_values(hp).start()

    def own_part(hp, before, whole):
        slot = lax.rem(hp, 2)
        strips = []
        for h in range(2):
            for n in range(2):
                at = slice(n * half, (n + 1) * half)
                parts = [(ks[hp, 0, h], vs[hp, 0, h], False)] if before else []
                mine = int(before)
                if n:
                    parts.append((ks[hp, mine, h, :half], vs[hp, mine, h, :, :half], False))
                parts.append((ks[hp, mine, h, at], vs[hp, mine, h, :, at], True))
                if whole and h:
                    parts += [(kx[i], vx[i], False) for i in range(2)]

                def put(out, top, total, h=h, at=at):
                    part[slot, h, :, at], tops[slot, h, :, at], sums[slot, h, :, at] = out, top, total

                strips.append((qs[hp, h, :, at], parts, put))
        attend(strips)

    def other_part(hp):
        strips = []
        for j in range(2):
            for n in range(2):
                at = slice(n * half, (n + 1) * half)

                def put(out, top, total, j=j, at=at):
                    outbox[hp, j, :, at] = (out * (1 / total)).astype(BF16)
                    lout[hp, j, :, at] = top + jnp.log2(total)

                strips.append((inbox[hp, j, :, at], [(ks[hp, n, core], vs[hp, n, core], False) for n in range(2)], put))
        attend(strips)

    def own_parts(hp, whole=False):
        @pl.when(core == 0)
        def _():
            own_part(hp, False, whole)

        @pl.when(core == 1)
        def _():
            own_part(hp, True, whole)

    def alone(hp, h):
        slot = lax.rem(hp, 2)
        seen[:, h * HEAD : (h + 1) * HEAD] = (part[slot, h] * (1 / sums[slot, h])).T.astype(BF16)

    def joined(hp, h):
        got(hp, h).wait_recv()
        got_sum(hp, h).wait_recv()
        slot = lax.rem(hp, 2)
        total = sums[slot, h]
        here, there = tops[slot, h] + jnp.log2(total), lin[hp, h]
        top = jnp.maximum(here, there)
        a, b = jnp.exp2(here - top), jnp.exp2(there - top)
        both = part[slot, h] * (a / (total * (a + b))) + inbox[hp, h].astype(F32) * (b / (a + b))
        seen[:, h * HEAD : (h + 1) * HEAD] = both.T.astype(BF16)

    def project(hp):
        rows(hp).wait()

        @pl.when(hp < pairs - 1)
        def _():
            for n in range(0, acc.shape[1], 512):
                acc[:, n : n + 512] += dot(seen[...], wo[hp, :, n : n + 512])

        @pl.when(hp == pairs - 1)
        def _():
            for n in range(0, acc.shape[1], 512):
                y_ref[:, n : n + 512] = (acc[:, n : n + 512] + dot(seen[...], wo[hp, :, n : n + 512])).astype(BF16)

    last = pairs - 1

    def cross(i):
        src, dst = ((ks.at[last, core, 1], kx.at[core]), (vs.at[last, core, 1], vx.at[core]))[i]
        return remote(src, dst, cs.at[i], cr.at[i], 2 + core)

    def crossed(i):
        box = (kx, vx)[i].at[core]
        return remote(box, box, cs.at[i], cr.at[i], core)

    def hand(i, whose):
        box = (kx, vx)[i].at[whose]
        return remote(box, box, fs.at[i], fr.at[i], sibling)

    @pl.when(first)
    def _():
        ahead = pairs - 3
        key_value(last, None)
        for i in range(2):
            cross(i).start()
        lax.fori_loop(0, ahead, key_value, None)

        def due(t):
            return t + lax.div(t, 5)

        def body(t, _):
            send_keys(t).wait_recv()
            send_values(t).wait_recv()

            @pl.when((t < last) | ((t == last) & (core == 0)))
            def _():
                for j in range(2):
                    got(t, j).wait_recv()
                other_part(t)
                for j in range(2):
                    send_part(t, j).start()
                    send_sum(t, j).start()

            @pl.when(t == 0)
            def _():
                lax.fori_loop(ahead, last, key_value, None)

            def mine(i, _):
                hp = due(t - 1) + i

                @pl.when((t > 0) & (hp < due(t)))
                def _():
                    own_parts(hp)
                    for h in range(2):
                        alone(hp, h)
                    project(hp)

            def ask(i, _):
                hp = 2 * t - 1 + i

                @pl.when((hp >= 0) & (hp < pairs))
                def _():
                    query(hp)

            lax.fori_loop(0, 2, mine, None)
            lax.fori_loop(0, 2, ask, None)

        lax.fori_loop(0, pairs, body, None)

    @pl.when(second)
    def _():
        def ask(hp, _):
            query(hp)
            send_query(hp, 0).start()

            @pl.when(hp < last)
            def _():
                send_query(hp, 1).start()

        lax.fori_loop(0, pairs, ask, None)
        lax.fori_loop(0, pairs, key_value, None)
        for i in range(2):
            crossed(i).wait_recv()
            hand(i, core).start()

        def here(hp):
            @pl.when(core == 1)
            def _():
                send_keys(hp).wait_recv()
                send_values(hp).wait_recv()

            @pl.when(hp < last)
            def _():
                own_parts(hp)

            @pl.when(hp == last)
            def _():
                for i in range(2):
                    hand(i, 1 - core).wait_recv()
                own_parts(hp, True)

        def body(t, _):
            hp = t - 1

            @pl.when(t < pairs)
            def _():
                here(t)

            @pl.when((t > 0) & (t < pairs))
            def _():
                joined(hp, 0)
                joined(hp, 1)
                project(hp)

            @pl.when(t == pairs)
            def _():
                alone(hp, 1)
                joined(hp, 0)
                project(hp)

        lax.fori_loop(0, pairs + 1, body, None)

    def finish(hp, _):
        @pl.when(sends_keys)
        def _():
            send_keys(hp).wait_send()
            send_values(hp).wait_send()

        for j in range(2):
            @pl.when(first & ((hp < last) | (core == 0)))
            def _():
                send_part(hp, j).wait_send()
                send_sum(hp, j).wait_send()

            @pl.when(second & ((hp < last) | (j == 0)))
            def _():
                send_query(hp, j).wait_send()

    lax.fori_loop(0, pairs, finish, None)
    for i in range(2):
        @pl.when(first)
        def _():
            cross(i).wait_send()

        @pl.when(second)
        def _():
            hand(i, core).wait_send()


def turning(tokens):
    half = HEAD // 2
    angle = np.arange(tokens)[:, None] * float(THETA) ** (-np.arange(half) / half)
    return np.concatenate([np.cos(angle), np.sin(angle)], -1).astype(np.float32)


def solution(mesh):
    devices = mesh.shape["sp"]

    def step(x, gain, wq, wk, wv, wo):
        own, width = x.shape
        pairs = wq.shape[1] // PAIR
        anywhere, vmem = pl.BlockSpec(memory_space=pl.ANY), pl.BlockSpec(memory_space=pltpu.VMEM)
        dma = lambda *shape: pltpu.SemaphoreType.DMA(shape)
        flops = 2 * own * width * 4 * width + 4 * own * own * devices * width
        return pl.pallas_call(
            kernel,
            out_shape=pltpu.VMEM((own, width), BF16),
            in_specs=[anywhere] * 7,
            out_specs=vmem,
            scratch_shapes=[
                pltpu.VMEM((own, width), BF16),
                pltpu.VMEM((own, width), BF16),
                pltpu.VMEM((width,), BF16),
                pltpu.VMEM((pairs, width, PAIR), BF16),
                pltpu.VMEM((pairs, width, PAIR), BF16),
                pltpu.VMEM((pairs, width, PAIR), BF16),
                pltpu.VMEM((pairs, PAIR, width), BF16),
                pltpu.VMEM((pairs, 2, 2, own, HEAD), BF16),
                pltpu.VMEM((pairs, 2, 2, HEAD, own), BF16),
                pltpu.VMEM((pairs, 2, HEAD, own), BF16),
                pltpu.VMEM((pairs, 2, HEAD, own), BF16),
                pltpu.VMEM((pairs, 2, HEAD, own), BF16),
                pltpu.VMEM((pairs, 2, 1, own), F32),
                pltpu.VMEM((pairs, 2, 1, own), F32),
                pltpu.VMEM((own, width), F32),
                pltpu.VMEM((2, own, HEAD), F32),
                pltpu.VMEM((2, 2, HEAD, own), F32),
                pltpu.VMEM((2, 2, 1, own), F32),
                pltpu.VMEM((2, 2, 1, own), F32),
                pltpu.VMEM((own, PAIR), BF16),
                dma(4, pairs), dma(own // CHUNK), dma(2), dma(pairs, 2), dma(pairs, 2), dma(pairs, 2), dma(pairs, 2), dma(pairs), dma(pairs), dma(pairs), dma(pairs),
                pltpu.VMEM((2, own, HEAD), BF16),
                pltpu.VMEM((2, HEAD, own), BF16),
                dma(2), dma(2), dma(2), dma(2),
            ],
            compiler_params=pltpu.CompilerParams(collective_id=0, has_side_effects=True, vmem_limit_bytes=123 * 2**19),
            cost_estimate=pl.CostEstimate(flops=flops, transcendentals=own * own * 2 * pairs * 2, bytes_accessed=4 * width * width * 2),
        )(x, gain, jnp.asarray(turning(devices * own)), wq, wk, wv, wo)

    tokens, whole = P(("dp", "sp"), None), P(None, None)
    return jax.shard_map(
        step,
        mesh=mesh,
        in_specs=(tokens, P(None), whole, whole, whole, whole),
        out_specs=tokens,
        check_vma=False,
    )
```

```python
import functools

import jax
import jax.numpy as jnp
import numpy as np
from jax import lax
from jax.experimental import pallas as pl
from jax.experimental.pallas import tpu as pltpu
from jax.sharding import PartitionSpec as P

HEAD = 128
THETA = 10000
PAIR = 2 * HEAD
LOG2E = 1.4426950408889634
E = HEAD**-0.5 * LOG2E
HIDDEN = -1e30
CHUNK, ROWS = 128, 16
F32, BF16 = jnp.float32, jnp.bfloat16
MESH = pl.DeviceIdType.MESH


def dot(a, b):
    return jnp.dot(a, b, preferred_element_type=F32)


def scores(q, parts):
    found = []
    for k, _, causal in parts:
        s = dot(k, q)
        if causal:
            s = jnp.where(lax.broadcasted_iota(jnp.int32, s.shape, 0) <= lax.broadcasted_iota(jnp.int32, s.shape, 1), s, HIDDEN)
        found.append(s)
    return found


def attend(strips):
    found = [scores(q, parts) for q, parts, _ in strips]
    tops = [functools.reduce(jnp.maximum, [s.max(axis=0, keepdims=True) for s in mine]) for mine in found]
    weights = [[jnp.exp2((s - top) * E).astype(BF16) for s in mine] for mine, top in zip(found, tops)]
    for (_, parts, put), top, mine in zip(strips, tops, weights):
        out = sum(dot(jnp.concatenate([v, jnp.ones((8, v.shape[1]), BF16)], axis=0), p) for (_, v, _), p in zip(parts, mine))
        put(out[:HEAD], top * E, out[HEAD : HEAD + 1])


def kernel(x_hbm, gain_hbm, turn_hbm, wq_hbm, wk_hbm, wv_hbm, wo_hbm, y_ref, xv, av, gv, wq, wk, wv, wo, ks, vs, qs, inbox, outbox, lin, lout, acc, turn, part,
           tops, sums, seen, w_sem, x_sem, m_sem, xs, xr, ls, lr, ss, sr, kx, vx, far):
    own, pairs = xv.shape[0], wq.shape[0]
    me = lax.axis_index("sp")
    chip, core = lax.div(me, 2), lax.rem(me, 2)
    sibling = 2 * chip + 1 - core
    first, second = chip == 0, chip == 1
    half = own // 2
    last = pairs - 1

    barrier = pltpu.get_barrier_semaphore()
    others = [lax.rem(me + n, 4) for n in (1, 2, 3)]
    for other in others:
        pl.semaphore_signal(barrier, inc=1, device_id={"sp": other}, device_id_type=MESH)

    def columns(w_hbm, w, i, hp):
        return pltpu.make_async_copy(w_hbm.at[:, pl.ds(pl.multiple_of(hp * PAIR, PAIR), PAIR)], w.at[hp], w_sem.at[i, hp])

    get_o = pltpu.make_async_copy(wo_hbm, wo, m_sem.at[2])
    get_q, get_k, get_v = (functools.partial(columns, *t) for t in ((wq_hbm, wq, 0), (wk_hbm, wk, 1), (wv_hbm, wv, 1)))
    def get_x(i):
        at = pl.ds(pl.multiple_of(i * CHUNK, CHUNK), CHUNK)
        return pltpu.make_async_copy(x_hbm.at[at, :], xv.at[at, :], x_sem.at[i])

    get_turn = pltpu.make_async_copy(turn_hbm.at[pl.ds(pl.multiple_of(me * own, own), own), :], turn.at[0], m_sem.at[1])
    for i in range(own // CHUNK):
        get_x(i).start()
    get_gain = pltpu.make_async_copy(gain_hbm, gv, m_sem.at[0])
    get_gain.start()
    get_turn.start()

    def start_all(count, *gets):
        def body(hp, _):
            for get in gets:
                get(hp).start()
        lax.fori_loop(0, count, body, None)

    @pl.when(first)
    def _():
        for get in (get_k, get_v):
            get(pairs - 1).start()
        start_all(pairs - 1, get_k, get_v)
        start_all(pairs, get_q)

    @pl.when(second)
    def _():
        start_all(pairs, get_q)
        start_all(pairs, get_k, get_v)

    get_o.start()

    get_gain.wait()

    def norm(i, _):
        get_x(i).wait()
        for n in range(0, CHUNK, ROWS):
            at = pl.ds(pl.multiple_of(i * CHUNK + n, ROWS), ROWS)
            wide = xv[at, :].astype(F32)
            scale = lax.rsqrt(jnp.mean(wide * wide, -1, keepdims=True) + 1e-6)
            av[at, :] = (wide * scale * gv[...].astype(F32).reshape(1, -1)).astype(BF16)

    lax.fori_loop(0, own // CHUNK, norm, None)

    get_turn.wait()
    table = turn[0]
    swapped = pltpu.roll(table, HEAD // 2, 1)
    low = lax.broadcasted_iota(jnp.int32, table.shape, 1) < HEAD // 2
    turn[0] = jnp.where(low, table, swapped)
    turn[1] = jnp.where(low, -swapped, table)

    pl.semaphore_wait(barrier, 3)

    def turned(t):
        wide = t.astype(F32)
        return (wide * turn[0] + pltpu.roll(wide, HEAD // 2, 1) * turn[1]).astype(BF16)

    def remote(src, dst, send, recv, device):
        return pltpu.make_async_remote_copy(src_ref=src, dst_ref=dst, send_sem=send, recv_sem=recv, device_id={"sp": device}, device_id_type=MESH)

    def late(hp):
        return lax.div(hp, last)

    def send_query(hp, j):
        return remote(qs.at[hp, j], inbox.at[hp, core], xs.at[late(hp)], xr.at[hp, core], j)

    def send_part(hp, j):
        return remote(outbox.at[hp, j], inbox.at[hp, core], xs.at[late(hp)], xr.at[hp, core], 2 + j)

    def send_sum(hp, j):
        return remote(lout.at[hp, j], lin.at[hp, core], ls.at[late(hp)], lr.at[hp, core], 2 + j)

    def got(hp, j):
        return remote(inbox.at[hp, j], inbox.at[hp, j], xs.at[0], xr.at[hp, j], 2 * (1 - chip) + j)

    def got_sum(hp, j):
        return remote(lin.at[hp, j], lin.at[hp, j], ls.at[0], lr.at[hp, j], 2 * (1 - chip) + j)

    def beside(box, hp):
        return remote(box, box, ss.at[0], sr.at[hp], sibling)

    def share(hp):
        for box in (ks, vs):
            @pl.when(core == 0)
            def _():
                beside(box.at[hp, core], hp).start()

            @pl.when(first & (core == 1))
            def _():
                beside(box.at[hp, core, 0], hp).start()

    def shared(hp):
        @pl.when(core == 1)
        def _():
            beside(ks.at[hp], hp).wait_recv()

        @pl.when(first & (core == 0))
        def _():
            beside(ks.at[hp, 1], hp).wait_recv()

    def query(hp):
        get_q(hp).wait()
        t = dot(av[...], wq[hp]).astype(BF16)
        for h in range(2):
            qs[hp, h] = turned(t[:, h * HEAD : (h + 1) * HEAD]).T

    def key_value(hp, _):
        two = wk.at[pl.ds(0, 2)]
        pltpu.make_async_copy(two, two, w_sem.at[1, hp]).wait()
        t = dot(av[...], wk[hp]).astype(BF16)
        for h in range(2):
            ks[hp, core, h] = turned(t[:, h * HEAD : (h + 1) * HEAD])
        t = dot(av[...], wv[hp]).astype(BF16)
        for h in range(2):
            vs[hp, core, h] = t[:, h * HEAD : (h + 1) * HEAD].T

        share(hp)

    def own_part(hp, before, whole):
        slot = lax.rem(hp, 2)
        strips = []
        for h in range(2):
            for n in range(2):
                at = slice(n * half, (n + 1) * half)
                parts = [(ks[hp, 0, h], vs[hp, 0, h], False)] if before else []
                mine = int(before)
                if n:
                    parts.append((ks[hp, mine, h, :half], vs[hp, mine, h, :, :half], False))
                parts.append((ks[hp, mine, h, at], vs[hp, mine, h, :, at], True))
                if whole and h:
                    parts += [(kx[i], vx[i], False) for i in range(2)]

                def put(out, top, total, h=h, at=at):
                    part[slot, h, :, at], tops[slot, h, :, at], sums[slot, h, :, at] = out, top, total

                strips.append((qs[hp, h, :, at], parts, put))
        attend(strips)

    def other_part(hp):
        strips = []
        for j in range(2):
            for n in range(2):
                at = slice(n * half, (n + 1) * half)

                def put(out, top, total, j=j, at=at):
                    outbox[hp, j, :, at] = (out * (1 / total)).astype(BF16)
                    lout[hp, j, :, at] = top + jnp.log2(total)

                strips.append((inbox[hp, j, :, at], [(ks[hp, n, core], vs[hp, n, core], False) for n in range(2)], put))
        attend(strips)

    def own_parts(hp, whole=False):
        @pl.when(core == 0)
        def _():
            own_part(hp, False, whole)

        @pl.when(core == 1)
        def _():
            own_part(hp, True, whole)

    def alone(hp, h):
        slot = lax.rem(hp, 2)
        seen[:, h * HEAD : (h + 1) * HEAD] = (part[slot, h] * (1 / sums[slot, h])).T.astype(BF16)

    def joined(hp, h):
        got(hp, h).wait_recv()
        got_sum(hp, h).wait_recv()
        slot = lax.rem(hp, 2)
        total = sums[slot, h]
        here, there = tops[slot, h] + jnp.log2(total), lin[hp, h]
        top = jnp.maximum(here, there)
        a, b = jnp.exp2(here - top), jnp.exp2(there - top)
        both = part[slot, h] * (a / (total * (a + b))) + inbox[hp, h].astype(F32) * (b / (a + b))
        seen[:, h * HEAD : (h + 1) * HEAD] = both.T.astype(BF16)

    def project(hp):
        def part_of(n):
            return dot(seen[...], wo[pl.ds(pl.multiple_of(hp * PAIR, PAIR), PAIR), n : n + 512])

        @pl.when(hp == 0)
        def _():
            get_o.wait()
            for n in range(0, acc.shape[1], 512):
                acc[:, n : n + 512] = xv[:, n : n + 512].astype(F32) + part_of(n)

        @pl.when((hp > 0) & (hp < last))
        def _():
            for n in range(0, acc.shape[1], 512):
                acc[:, n : n + 512] += part_of(n)

        @pl.when(hp == last)
        def _():
            for n in range(0, acc.shape[1], 512):
                y_ref[:, n : n + 512] = (acc[:, n : n + 512] + part_of(n)).astype(BF16)


    def cross(i):
        src, dst = ((ks.at[last, core, 1], kx.at[core]), (vs.at[last, core, 1], vx.at[core]))[i]
        return remote(src, dst, far.at[0], far.at[1], 2 + core)

    def hand(i):
        box = (kx, vx)[i].at[core]
        return remote(box, box, far.at[2], far.at[3], sibling)

    crossed, handed = remote(kx, kx, far.at[0], far.at[1], core), remote(kx, kx, far.at[2], far.at[3], sibling)

    @pl.when(first)
    def _():
        ahead = pairs - 3
        key_value(last, None)
        for i in range(2):
            cross(i).start()
        lax.fori_loop(0, ahead, key_value, None)

        def due(t):
            return t + lax.div(t, 5)

        def body(t, _):
            shared(t)

            @pl.when((t < last) | ((t == last) & (core == 0)))
            def _():
                for j in range(2):
                    got(t, j).wait_recv()
                other_part(t)
                for j in range(2):
                    send_part(t, j).start()
                    send_sum(t, j).start()

            @pl.when(t == 0)
            def _():
                lax.fori_loop(ahead, last, key_value, None)

            def mine(i, _):
                hp = due(t - 1) + i

                @pl.when((t > 0) & (hp < due(t)))
                def _():
                    own_parts(hp)
                    for h in range(2):
                        alone(hp, h)
                    project(hp)

            def ask(i, _):
                hp = 2 * t - 1 + i

                @pl.when((hp >= 0) & (hp < pairs))
                def _():
                    query(hp)

            lax.fori_loop(0, 2, mine, None)
            lax.fori_loop(0, 2, ask, None)

        lax.fori_loop(0, pairs, body, None)

    @pl.when(second)
    def _():
        def ask(hp, _):
            query(hp)
            send_query(hp, 0).start()

            @pl.when(hp < last)
            def _():
                send_query(hp, 1).start()

        lax.fori_loop(0, pairs, ask, None)
        lax.fori_loop(0, pairs, key_value, None)
        crossed.wait_recv()
        for i in range(2):
            hand(i).start()

        def here(hp):
            shared(hp)

            @pl.when(hp < last)
            def _():
                own_parts(hp)

            @pl.when(hp == last)
            def _():
                handed.wait_recv()
                own_parts(hp, True)

        def body(t, _):
            hp = t - 1

            @pl.when(t < pairs)
            def _():
                here(t)

            @pl.when((t > 0) & (t < pairs))
            def _():
                joined(hp, 0)
                joined(hp, 1)
                project(hp)

            @pl.when(t == pairs)
            def _():
                alone(hp, 1)
                joined(hp, 0)
                project(hp)

        lax.fori_loop(0, pairs + 1, body, None)

    most, rest, sums_of = outbox.at[pl.ds(0, last)], outbox.at[last], lout.at[pl.ds(0, last)]
    remote(most, most, xs.at[0], xr.at[0, 0], sibling).wait_send()

    @pl.when(first)
    def _():
        remote(sums_of, sums_of, ls.at[0], lr.at[0, 0], sibling).wait_send()
        crossed.wait_send()

    @pl.when(first & (core == 0))
    def _():
        remote(rest, rest, xs.at[1], xr.at[0, 0], sibling).wait_send()
        remote(lout.at[last], lout.at[last], ls.at[1], lr.at[0, 0], sibling).wait_send()

    @pl.when(second)
    def _():
        remote(rest.at[0], rest.at[0], xs.at[1], xr.at[0, 0], sibling).wait_send()
        handed.wait_send()

    @pl.when(core == 0)
    def _():
        beside(ks, 0).wait_send()

    @pl.when(first & (core == 1))
    def _():
        beside(ks.at[:, 0], 0).wait_send()


def turning(tokens):
    half = HEAD // 2
    angle = np.arange(tokens)[:, None] * float(THETA) ** (-np.arange(half) / half)
    return np.concatenate([np.cos(angle), np.sin(angle)], -1).astype(np.float32)


def solution(mesh):
    devices = mesh.shape["sp"]

    def step(x, gain, wq, wk, wv, wo):
        own, width = x.shape
        pairs = wq.shape[1] // PAIR
        anywhere, vmem = pl.BlockSpec(memory_space=pl.ANY), pl.BlockSpec(memory_space=pltpu.VMEM)
        dma = lambda *shape: pltpu.SemaphoreType.DMA(shape)
        flops = 2 * own * width * 4 * width + 4 * own * own * devices * width
        return pl.pallas_call(
            kernel,
            out_shape=pltpu.VMEM((own, width), BF16),
            in_specs=[anywhere] * 7,
            out_specs=vmem,
            scratch_shapes=[
                pltpu.VMEM((own, width), BF16),
                pltpu.VMEM((own, width), BF16),
                pltpu.VMEM((width,), BF16),
                pltpu.VMEM((pairs, width, PAIR), BF16),
                pltpu.VMEM((pairs, width, PAIR), BF16),
                pltpu.VMEM((pairs, width, PAIR), BF16),
                pltpu.VMEM((width, width), BF16),
                pltpu.VMEM((pairs, 2, 2, own, HEAD), BF16),
                pltpu.VMEM((pairs, 2, 2, HEAD, own), BF16),
                pltpu.VMEM((pairs, 2, HEAD, own), BF16),
                pltpu.VMEM((pairs, 2, HEAD, own), BF16),
                pltpu.VMEM((pairs, 2, HEAD, own), BF16),
                pltpu.VMEM((pairs, 2, 1, own), F32),
                pltpu.VMEM((pairs, 2, 1, own), F32),
                pltpu.VMEM((own, width), F32),
                pltpu.VMEM((2, own, HEAD), F32),
                pltpu.VMEM((2, 2, HEAD, own), F32),
                pltpu.VMEM((2, 2, 1, own), F32),
                pltpu.VMEM((2, 2, 1, own), F32),
                pltpu.VMEM((own, PAIR), BF16),
                dma(2, pairs), dma(own // CHUNK), dma(3), dma(2), dma(pairs, 2), dma(2), dma(pairs, 2), dma(1), dma(pairs),
                pltpu.VMEM((2, own, HEAD), BF16),
                pltpu.VMEM((2, HEAD, own), BF16),
                dma(4),
            ],
            compiler_params=pltpu.CompilerParams(collective_id=0, has_side_effects=True, vmem_limit_bytes=123 * 2**19),
            cost_estimate=pl.CostEstimate(flops=flops, transcendentals=own * own * 2 * pairs * 2, bytes_accessed=4 * width * width * 2),
        )(x, gain, jnp.asarray(turning(devices * own)), wq, wk, wv, wo)

    tokens, whole = P(("dp", "sp"), None), P(None, None)
    return jax.shard_map(
        step,
        mesh=mesh,
        in_specs=(tokens, P(None), whole, whole, whole, whole),
        out_specs=tokens,
        check_vma=False,
    )
```

```python
import functools

import jax
import jax.numpy as jnp
import numpy as np
from jax import lax
from jax.experimental import pallas as pl
from jax.experimental.pallas import tpu as pltpu
from jax.sharding import PartitionSpec as P

HEAD = 128
THETA = 10000
PAIR = 2 * HEAD
LOG2E = 1.4426950408889634
E = HEAD**-0.5 * LOG2E
HIDDEN = -1e30
CHUNK, ROWS = 128, 16
F32, BF16 = jnp.float32, jnp.bfloat16
MESH = pl.DeviceIdType.MESH


def dot(a, b):
    return jnp.dot(a, b, preferred_element_type=F32)


def scores(q, parts):
    found = []
    for k, _, causal in parts:
        s = dot(k, q)
        if causal:
            s = jnp.where(lax.broadcasted_iota(jnp.int32, s.shape, 0) <= lax.broadcasted_iota(jnp.int32, s.shape, 1), s, HIDDEN)
        found.append(s)
    return found


def attend(strips):
    found = [scores(q, parts) for q, parts, _ in strips]
    tops = [functools.reduce(jnp.maximum, [s.max(axis=0, keepdims=True) for s in mine]) for mine in found]
    weights = [[jnp.exp2((s - top) * E).astype(BF16) for s in mine] for mine, top in zip(found, tops)]
    for (_, parts, put), top, mine in zip(strips, tops, weights):
        out = sum(dot(jnp.concatenate([v, jnp.ones((8, v.shape[1]), BF16)], axis=0), p) for (_, v, _), p in zip(parts, mine))
        put(out[:HEAD], top * E, out[HEAD : HEAD + 1])


def kernel(x_hbm, gain_hbm, turn_hbm, wq_hbm, wk_hbm, wv_hbm, wo_hbm, y_ref, xv, av, gv, wq, wk, wv, wo, ks, vs, qs, inbox, outbox, lin, lout, acc, turn, part,
           tops, sums, seen, w_sem, x_sem, m_sem, xs, xr, ls, lr, ss, sr, kx, vx, far):
    own, pairs = xv.shape[0], wq.shape[0]
    me = lax.axis_index("sp")
    chip, core = lax.div(me, 2), lax.rem(me, 2)
    sibling = 2 * chip + 1 - core
    first, second = chip == 0, chip == 1
    half = own // 2
    last = pairs - 1

    barrier = pltpu.get_barrier_semaphore()
    others = [lax.rem(me + n, 4) for n in (1, 2, 3)]
    for other in others:
        pl.semaphore_signal(barrier, inc=1, device_id={"sp": other}, device_id_type=MESH)

    def columns(w_hbm, w, i, hp):
        return pltpu.make_async_copy(w_hbm.at[:, pl.ds(pl.multiple_of(hp * PAIR, PAIR), PAIR)], w.at[hp], w_sem.at[i, hp])

    get_o = pltpu.make_async_copy(wo_hbm, wo, m_sem.at[2])
    get_q, get_k, get_v = (functools.partial(columns, *t) for t in ((wq_hbm, wq, 0), (wk_hbm, wk, 1), (wv_hbm, wv, 1)))
    def get_x(i):
        at = pl.ds(pl.multiple_of(i * CHUNK, CHUNK), CHUNK)
        return pltpu.make_async_copy(x_hbm.at[at, :], xv.at[at, :], x_sem.at[i])

    get_turn = pltpu.make_async_copy(turn_hbm.at[pl.ds(pl.multiple_of(me * own, own), own), :], turn.at[0], m_sem.at[1])
    for i in range(own // CHUNK):
        get_x(i).start()
    get_gain = pltpu.make_async_copy(gain_hbm, gv, m_sem.at[0])
    get_gain.start()
    get_turn.start()

    def start_all(count, *gets):
        def body(hp, _):
            for get in gets:
                get(hp).start()
        lax.fori_loop(0, count, body, None)

    @pl.when(first)
    def _():
        for get in (get_k, get_v):
            get(pairs - 1).start()
        start_all(pairs - 1, get_k, get_v)
        start_all(pairs, get_q)

    @pl.when(second)
    def _():
        start_all(pairs, get_q)
        start_all(pairs, get_k, get_v)

    get_o.start()

    get_gain.wait()

    def norm(i, _):
        get_x(i).wait()
        for n in range(0, CHUNK, ROWS):
            at = pl.ds(pl.multiple_of(i * CHUNK + n, ROWS), ROWS)
            wide = xv[at, :].astype(F32)
            scale = lax.rsqrt(jnp.mean(wide * wide, -1, keepdims=True) + 1e-6)
            av[at, :] = (wide * scale * gv[...].astype(F32).reshape(1, -1)).astype(BF16)

    lax.fori_loop(0, own // CHUNK, norm, None)

    get_turn.wait()
    table = turn[0]
    swapped = pltpu.roll(table, HEAD // 2, 1)
    low = lax.broadcasted_iota(jnp.int32, table.shape, 1) < HEAD // 2
    turn[0] = jnp.where(low, table, swapped)
    turn[1] = jnp.where(low, -swapped, table)

    pl.semaphore_wait(barrier, 3)

    def turned(t):
        wide = t.astype(F32)
        return (wide * turn[0] + pltpu.roll(wide, HEAD // 2, 1) * turn[1]).astype(BF16)

    def remote(src, dst, send, recv, device):
        return pltpu.make_async_remote_copy(src_ref=src, dst_ref=dst, send_sem=send, recv_sem=recv, device_id={"sp": device}, device_id_type=MESH)

    def late(hp):
        return lax.div(hp, last)

    def send_query(hp, j):
        return remote(qs.at[hp, j], inbox.at[hp, core], xs.at[late(hp)], xr.at[hp, core], j)

    def send_part(hp, j):
        return remote(outbox.at[hp, j], inbox.at[hp, core], xs.at[late(hp)], xr.at[hp, core], 2 + j)

    def send_sum(hp, j):
        return remote(lout.at[hp, j], lin.at[hp, core], ls.at[late(hp)], lr.at[hp, core], 2 + j)

    def got(hp, j):
        return remote(inbox.at[hp, j], inbox.at[hp, j], xs.at[0], xr.at[hp, j], 2 * (1 - chip) + j)

    def got_sum(hp, j):
        return remote(lin.at[hp, j], lin.at[hp, j], ls.at[0], lr.at[hp, j], 2 * (1 - chip) + j)

    def beside(box, hp):
        return remote(box, box, ss.at[0], sr.at[hp], sibling)

    def share(hp):
        for box in (ks, vs):
            @pl.when(core == 0)
            def _():
                beside(box.at[hp, core], hp).start()

            @pl.when(first & (core == 1))
            def _():
                beside(box.at[hp, core, 0], hp).start()

    def shared(hp):
        @pl.when(core == 1)
        def _():
            beside(ks.at[hp], hp).wait_recv()

        @pl.when(first & (core == 0))
        def _():
            beside(ks.at[hp, 1], hp).wait_recv()

    def query(hp):
        get_q(hp).wait()
        t = dot(av[...], wq[hp]).astype(BF16)
        for h in range(2):
            qs[hp, h] = turned(t[:, h * HEAD : (h + 1) * HEAD]).T

    def key_value(hp, _):
        two = wk.at[pl.ds(0, 2)]
        pltpu.make_async_copy(two, two, w_sem.at[1, hp]).wait()
        t = dot(av[...], wk[hp]).astype(BF16)
        for h in range(2):
            ks[hp, core, h] = turned(t[:, h * HEAD : (h + 1) * HEAD])
        t = dot(av[...], wv[hp]).astype(BF16)
        for h in range(2):
            vs[hp, core, h] = t[:, h * HEAD : (h + 1) * HEAD].T

        share(hp)

    def own_part(hp, before, whole):
        slot = lax.rem(hp, 2)
        strips = []
        for h in range(2):
            for n in range(2):
                at = slice(n * half, (n + 1) * half)
                parts = [(ks[hp, 0, h], vs[hp, 0, h], False)] if before else []
                mine = int(before)
                if n:
                    parts.append((ks[hp, mine, h, :half], vs[hp, mine, h, :, :half], False))
                parts.append((ks[hp, mine, h, at], vs[hp, mine, h, :, at], True))
                if whole and h:
                    parts += [(kx[i], vx[i], False) for i in range(2)]

                def put(out, top, total, h=h, at=at):
                    part[slot, h, :, at], tops[slot, h, :, at], sums[slot, h, :, at] = out, top, total

                strips.append((qs[hp, h, :, at], parts, put))
        attend(strips)

    def other_part(hp):
        strips = []
        for j in range(2):
            for n in range(2):
                at = slice(n * half, (n + 1) * half)

                def put(out, top, total, j=j, at=at):
                    outbox[hp, j, :, at] = (out * (1 / total)).astype(BF16)
                    lout[hp, j, :, at] = top + jnp.log2(total)

                strips.append((inbox[hp, j, :, at], [(ks[hp, n, core], vs[hp, n, core], False) for n in range(2)], put))
        attend(strips)

    def own_parts(hp, whole=False):
        @pl.when(core == 0)
        def _():
            own_part(hp, False, whole)

        @pl.when(core == 1)
        def _():
            own_part(hp, True, whole)

    def alone(hp, h):
        slot = lax.rem(hp, 2)
        seen[:, h * HEAD : (h + 1) * HEAD] = (part[slot, h] * (1 / sums[slot, h])).T.astype(BF16)

    def joined(hp, h):
        got(hp, h).wait_recv()
        got_sum(hp, h).wait_recv()
        slot = lax.rem(hp, 2)
        total = sums[slot, h]
        here, there = tops[slot, h] + jnp.log2(total), lin[hp, h]
        top = jnp.maximum(here, there)
        a, b = jnp.exp2(here - top), jnp.exp2(there - top)
        both = part[slot, h] * (a / (total * (a + b))) + inbox[hp, h].astype(F32) * (b / (a + b))
        seen[:, h * HEAD : (h + 1) * HEAD] = both.T.astype(BF16)

    def project(hp):
        def part_of(n):
            return dot(seen[...], wo[pl.ds(pl.multiple_of(hp * PAIR, PAIR), PAIR), n : n + 512])

        @pl.when(hp == 0)
        def _():
            get_o.wait()
            for n in range(0, acc.shape[1], 512):
                acc[:, n : n + 512] = xv[:, n : n + 512].astype(F32) + part_of(n)

        @pl.when((hp > 0) & (hp < last))
        def _():
            for n in range(0, acc.shape[1], 512):
                acc[:, n : n + 512] += part_of(n)

        @pl.when(hp == last)
        def _():
            for n in range(0, acc.shape[1], 512):
                y_ref[:, n : n + 512] = (acc[:, n : n + 512] + part_of(n)).astype(BF16)


    def cross(i):
        src, dst = ((ks.at[last, core, 1], kx.at[core]), (vs.at[last, core, 1], vx.at[core]))[i]
        return remote(src, dst, far.at[0], far.at[1], 2 + core)

    def hand(i):
        box = (kx, vx)[i].at[core]
        return remote(box, box, far.at[2], far.at[3], sibling)

    crossed, handed = remote(kx, kx, far.at[0], far.at[1], core), remote(kx, kx, far.at[2], far.at[3], sibling)

    @pl.when(first)
    def _():
        ahead, then = 4 + 2 * core, 6 + core
        key_value(last, None)
        for i in range(2):
            cross(i).start()
        lax.fori_loop(0, ahead, key_value, None)

        def due(t):
            return t + lax.div(t, 5)

        def body(t, _):
            shared(t)

            @pl.when((t < last) | ((t == last) & (core == 0)))
            def _():
                for j in range(2):
                    got(t, j).wait_recv()
                other_part(t)
                for j in range(2):
                    send_part(t, j).start()
                    send_sum(t, j).start()

            @pl.when(t == 0)
            def _():
                lax.fori_loop(ahead, then, key_value, None)

            @pl.when(t == 1)
            def _():
                lax.fori_loop(then, last, key_value, None)

            def mine(i, _):
                hp = due(t - 1) + i

                @pl.when((t > 0) & (hp < due(t)))
                def _():
                    own_parts(hp)
                    for h in range(2):
                        alone(hp, h)
                    project(hp)

            def ask(i, _):
                hp = 2 * t - 1 + i

                @pl.when((hp >= 0) & (hp < pairs))
                def _():
                    query(hp)

            lax.fori_loop(0, 2, mine, None)
            lax.fori_loop(0, 2, ask, None)

        lax.fori_loop(0, pairs, body, None)

    @pl.when(second)
    def _():
        def ask(hp, _):
            query(hp)
            send_query(hp, 0).start()

            @pl.when(hp < last)
            def _():
                send_query(hp, 1).start()

        lax.fori_loop(0, pairs, ask, None)
        lax.fori_loop(0, pairs, key_value, None)
        crossed.wait_recv()
        for i in range(2):
            hand(i).start()

        def here(hp):
            shared(hp)

            @pl.when(hp < last)
            def _():
                own_parts(hp)

            @pl.when(hp == last)
            def _():
                handed.wait_recv()
                own_parts(hp, True)

        def body(t, _):
            hp = t - 1

            @pl.when(t < pairs)
            def _():
                here(t)

            @pl.when((t > 0) & (t < pairs))
            def _():
                joined(hp, 0)
                joined(hp, 1)
                project(hp)

            @pl.when(t == pairs)
            def _():
                alone(hp, 1)
                joined(hp, 0)
                project(hp)

        lax.fori_loop(0, pairs + 1, body, None)

    most, rest, sums_of = outbox.at[pl.ds(0, last)], outbox.at[last], lout.at[pl.ds(0, last)]
    remote(most, most, xs.at[0], xr.at[0, 0], sibling).wait_send()

    @pl.when(first)
    def _():
        remote(sums_of, sums_of, ls.at[0], lr.at[0, 0], sibling).wait_send()
        crossed.wait_send()

    @pl.when(first & (core == 0))
    def _():
        remote(rest, rest, xs.at[1], xr.at[0, 0], sibling).wait_send()
        remote(lout.at[last], lout.at[last], ls.at[1], lr.at[0, 0], sibling).wait_send()

    @pl.when(second)
    def _():
        remote(rest.at[0], rest.at[0], xs.at[1], xr.at[0, 0], sibling).wait_send()
        handed.wait_send()

    @pl.when(core == 0)
    def _():
        beside(ks, 0).wait_send()

    @pl.when(first & (core == 1))
    def _():
        beside(ks.at[:, 0], 0).wait_send()


def turning(tokens):
    half = HEAD // 2
    angle = np.arange(tokens)[:, None] * float(THETA) ** (-np.arange(half) / half)
    return np.concatenate([np.cos(angle), np.sin(angle)], -1).astype(np.float32)


def solution(mesh):
    devices = mesh.shape["sp"]

    def step(x, gain, wq, wk, wv, wo):
        own, width = x.shape
        pairs = wq.shape[1] // PAIR
        anywhere, vmem = pl.BlockSpec(memory_space=pl.ANY), pl.BlockSpec(memory_space=pltpu.VMEM)
        dma = lambda *shape: pltpu.SemaphoreType.DMA(shape)
        flops = 2 * own * width * 4 * width + 4 * own * own * devices * width
        return pl.pallas_call(
            kernel,
            out_shape=pltpu.VMEM((own, width), BF16),
            in_specs=[anywhere] * 7,
            out_specs=vmem,
            scratch_shapes=[
                pltpu.VMEM((own, width), BF16),
                pltpu.VMEM((own, width), BF16),
                pltpu.VMEM((width,), BF16),
                pltpu.VMEM((pairs, width, PAIR), BF16),
                pltpu.VMEM((pairs, width, PAIR), BF16),
                pltpu.VMEM((pairs, width, PAIR), BF16),
                pltpu.VMEM((width, width), BF16),
                pltpu.VMEM((pairs, 2, 2, own, HEAD), BF16),
                pltpu.VMEM((pairs, 2, 2, HEAD, own), BF16),
                pltpu.VMEM((pairs, 2, HEAD, own), BF16),
                pltpu.VMEM((pairs, 2, HEAD, own), BF16),
                pltpu.VMEM((pairs, 2, HEAD, own), BF16),
                pltpu.VMEM((pairs, 2, 1, own), F32),
                pltpu.VMEM((pairs, 2, 1, own), F32),
                pltpu.VMEM((own, width), F32),
                pltpu.VMEM((2, own, HEAD), F32),
                pltpu.VMEM((2, 2, HEAD, own), F32),
                pltpu.VMEM((2, 2, 1, own), F32),
                pltpu.VMEM((2, 2, 1, own), F32),
                pltpu.VMEM((own, PAIR), BF16),
                dma(2, pairs), dma(own // CHUNK), dma(3), dma(2), dma(pairs, 2), dma(2), dma(pairs, 2), dma(1), dma(pairs),
                pltpu.VMEM((2, own, HEAD), BF16),
                pltpu.VMEM((2, HEAD, own), BF16),
                dma(4),
            ],
            compiler_params=pltpu.CompilerParams(collective_id=0, has_side_effects=True, vmem_limit_bytes=123 * 2**19),
            cost_estimate=pl.CostEstimate(flops=flops, transcendentals=own * own * 2 * pairs * 2, bytes_accessed=4 * width * width * 2),
        )(x, gain, jnp.asarray(turning(devices * own)), wq, wk, wv, wo)

    tokens, whole = P(("dp", "sp"), None), P(None, None)
    return jax.shard_map(
        step,
        mesh=mesh,
        in_specs=(tokens, P(None), whole, whole, whole, whole),
        out_specs=tokens,
        check_vma=False,
    )
```
